256 devices in a mesh: member: 2 (over z), lat: 16 (over x, core), lon: 8 (over y).
Axes of the slice: x: 8, y: 8, z: 2, core: 2. Of those that a mesh axis runs over, the one named last changes fastest.
The devices are a block of a 8x8x16 slice.
Arguments:
- field: bfloat16 [1024, 1024, 256], P(('member', 'lat'), 'lon'), parts along dimension 0, may hold values from -6 to 6
- mode_table: int32 [384], replicated, may hold values from 0 to 383, as said below
- analysis: bfloat16 [384, 384, 512], P(('lat', 'lon')), as said below
- synthesis: bfloat16 [384, 384, 512], P(('lat', 'lon')), as said below
- mixing: bfloat16 [1, 2, 256, 256], replicated, may hold values from -0.25 to 0.25
- degree_gain: float32 [1, 384, 256], replicated, may hold values from 0.25 to 1.75
- skip_weight: bfloat16 [1, 256, 256], replicated, may hold values from -0.375 to 0.375
Outputs:
- advanced: bfloat16 [1024, 1024, 256], P(('member', 'lat'), 'lon'), parts along dimension 0
- spectrum: bfloat16 [768, 384, 2, 256], P(('member', 'lat', 'lon')), parts along dimension 0
The draws below stay inside these ranges and needn't reach their ends.
There are 2 independent parts, one for each index of `member`. The reference program is written for one: setup_inputs(seed, part) draws one part's arguments, and reference() takes and returns one part's arrays. A program takes and returns all parts, laid end to end along the dimension named above; an argument that names none is the same for every part. Nothing has to cross between parts.
Inputs may be any that keep to these rules, and one draw needn't show every extreme that they name: A permutation of 0 to 383; slot s of the spectral layout holds zonal wavenumber mode_table[s]. analysis[s, l, j] = weight[j] P(l, m, colat[j]) rounded to bfloat16, with m = mode_table[s], colat[j] = pi (j + 0.5) / 512, weight[j] = 2 pi^2 sin(colat[j]) / 524288, and P the orthonormal associated Legendre function of degree l and order m at cos(colat) without the Condon-Shortley phase, zero for l < m. synthesis[s, l, j] = c P(l, m, colat[j]) rounded to bfloat16, with m = mode_table[s], c = 1 where m = 0 and c = 2 elsewhere, P and colat as for analysis.
All inputs are finite; a program needn't handle non-finite values.
Results may differ from the reference program's by a relative error of at most 0.0062.
Values may be sent and summed in bfloat16 or wider, within the bound.
No kernel may reach another device: no remote copies, remote signals or barrier semaphores. Data moves between devices by JAX's collectives and lax.ppermute only.
A program may use at most 64 MiB of HBM per device.

```python
import math
import jax
import jax.numpy as jnp
from jax import lax

C = 256
BLOCKS = 1
NLAT = 512
NLON = 1024
MMAX = 384


def table_orders(key):
    return jax.random.permutation(jax.random.fold_in(key, 11), MMAX).astype(jnp.int32)


def colatitudes(length):
    return (jnp.arange(length, dtype=jnp.float32) + 0.5) * (math.pi / length)


def legendre_values(orders):
    colatitude = colatitudes(NLAT)
    morder = orders.astype(jnp.float32)[:, None]
    cosine = jnp.cos(colatitude)[None, :]
    gamma_half = 0.5 * math.log(math.pi) - math.log(2.0)
    norm_part = 0.5 * (jax.scipy.special.gammaln(morder + 1.5) - jax.scipy.special.gammaln(morder + 1.0) - gamma_half)
    first_log = -0.5 * math.log(4.0 * math.pi) + norm_part + morder * jnp.log(jnp.sin(colatitude))[None, :]
    zero_state = jnp.zeros((orders.shape[0], NLAT), jnp.float32)

    def recur_step(carried, degree):
        upper_value, lower_value, log_scale = carried
        beyond = degree > morder
        starting = degree == morder
        square = degree * degree - morder * morder
        coef_first = jnp.sqrt(jnp.maximum(4.0 * degree * degree - 1.0, 1.0) / jnp.maximum(square, 1.0))
        previous = (degree - 1.0) * (degree - 1.0)
        coef_second = jnp.sqrt(jnp.maximum(previous - morder * morder, 0.0) / jnp.maximum(4.0 * previous - 1.0, 1.0))
        new_upper = jnp.where(beyond, coef_first * (cosine * upper_value - coef_second * lower_value), jnp.where(starting, 1.0, 0.0))
        new_lower = jnp.where(beyond, upper_value, 0.0)
        new_log = jnp.where(starting, first_log, log_scale)
        result = new_upper * jnp.exp(new_log)
        largest = jnp.maximum(jnp.abs(new_upper), jnp.abs(new_lower))
        largest = jnp.where(largest > 0, largest, 1.0)
        return ((new_upper / largest, new_lower / largest, new_log + jnp.log(largest)), result)
    _, values = lax.scan(recur_step, (zero_state, zero_state, zero_state), jnp.arange(MMAX, dtype=jnp.float32))
    return (jnp.transpose(values, (1, 0, 2)), colatitude)


def draw_mode_table(key, part):
    return table_orders(key)


def draw_analysis(key, part):
    values, colatitude = legendre_values(table_orders(key))
    weight = 2.0 * math.pi * math.pi / (NLON * NLAT) * jnp.sin(colatitude)
    return (values * weight[None, None, :]).astype(jnp.bfloat16)


def draw_synthesis(key, part):
    orders = table_orders(key)
    values, colatitude = legendre_values(orders)
    factor = jnp.where(orders == 0, 1.0, 2.0).astype(jnp.float32)
    return (values * factor[:, None, None]).astype(jnp.bfloat16)


def shard_levels(stream_key, dims, pieces, least, high):
    def one(position, blocks):
        steps = jax.random.uniform(jax.random.fold_in(jax.random.fold_in(stream_key, 6), position), (blocks,), jnp.float32, least / len(pieces), high / len(pieces))
        return jnp.repeat(jnp.exp(steps), dims[position] // blocks).reshape((-1,) + (1,) * (len(dims) - position - 1))

    loudness = one(*pieces[0])
    for cut in pieces[1:]:
        loudness = loudness * one(*cut)
    return loudness


def bell_draw(key, dims, width, reach, shards=(), kind=jnp.bfloat16):
    values = width * jax.random.normal(key, dims, jnp.float32)
    if shards:
        values = values * shard_levels(key, dims, shards, -0.22, 0.18)
    return jnp.clip(values, -reach, reach).astype(kind)


def setup_inputs(seed: int = 0, part: int = 0) -> dict:
    streams_of = jax.random.split(jax.random.key(seed), 8)
    part_keys = jax.random.split(jax.random.fold_in(streams_of[7], part), 8)
    return {
        "field": bell_draw(part_keys[0], (NLAT, NLON, C), 1.0, 6.0, ((0, 16), (1, 8))),
        "mode_table": draw_mode_table(jax.random.fold_in(streams_of[7], 71), part),
        "analysis": draw_analysis(jax.random.fold_in(streams_of[7], 71), part),
        "synthesis": draw_synthesis(jax.random.fold_in(streams_of[7], 71), part),
        "mixing": bell_draw(streams_of[4], (BLOCKS, 2, C, C), (2 * C) ** -0.5, 0.25),
        "degree_gain": jnp.clip(1.0 + 0.15 * jax.random.normal(streams_of[5], (BLOCKS, MMAX, C), jnp.float32), 0.25, 1.75),
        "skip_weight": bell_draw(streams_of[6], (BLOCKS, C, C), C ** -0.5, 0.375),
    }


def fourier_table(orders, length):
    phases = (orders[:, None] * jnp.arange(length, dtype=jnp.int32)[None, :]) % length
    angles = phases.astype(jnp.float32) * (2.0 * math.pi / length)
    return jnp.stack([jnp.cos(angles), -jnp.sin(angles)], axis=1).reshape(2 * orders.shape[0], length).astype(jnp.bfloat16)


def rounded(values):
    return lax.optimization_barrier(values.astype(jnp.bfloat16)).astype(jnp.float32)


def reference(field, mode_table, analysis, synthesis, mixing, degree_gain, skip_weight):
    highest = lax.Precision.HIGHEST
    orders = mode_table.astype(jnp.int32)
    analysis_wide = analysis.astype(jnp.float32)
    synthesis_wide = synthesis.astype(jnp.float32)
    table = lax.optimization_barrier(fourier_table(orders, NLON)).astype(jnp.float32)
    current = field
    mixed_modes = None
    for layer_index in range(BLOCKS):
        state_wide = current.astype(jnp.float32)
        lat_side = rounded(jnp.einsum("jkc,qk->jqc", state_wide, table, precision=highest))
        lat_data = lat_side.reshape(NLAT, MMAX, 2 * C)
        coefficients = rounded(jnp.einsum("slj,jsx->slx", analysis_wide, lat_data, precision=highest))
        real_part = mixing[layer_index, 0].astype(jnp.float32)
        imag_part = mixing[layer_index, 1].astype(jnp.float32)
        joined = jnp.concatenate([jnp.concatenate([real_part, imag_part], axis=1), jnp.concatenate([-imag_part, real_part], axis=1)], axis=0)
        product = jnp.dot(coefficients.reshape(-1, 2 * C), joined, precision=highest).reshape(MMAX, MMAX, 2, C)
        mixed_modes = (product * degree_gain[layer_index][None, :, None, :]).astype(jnp.bfloat16)
        synthesized = rounded(jnp.einsum("slj,slx->jsx", synthesis_wide, mixed_modes.astype(jnp.float32).reshape(MMAX, MMAX, 2 * C), precision=highest))
        synthesized = synthesized.reshape(NLAT, 2 * MMAX, C)
        spectral = rounded(jnp.einsum("jqc,qk->jkc", synthesized, table, precision=highest))
        direct = jnp.dot(current.reshape(-1, C), skip_weight[layer_index], preferred_element_type=jnp.float32).reshape(NLAT, NLON, C)
        current = (state_wide + jax.nn.gelu(spectral + direct, approximate=False)).astype(jnp.bfloat16)
    return current, mixed_modes
```

```python
import math

import jax
import jax.numpy as jnp
from jax import lax
from jax.sharding import Mesh, PartitionSpec as P

SWAP = [(0, 1), (1, 0)]
OWNERS = ("latx", "lon")


def fourier_table(orders, length):
    phases = orders[:, None] * jnp.arange(length, dtype=jnp.int32)[None, :] % length
    angles = phases.astype(jnp.float32) * (2.0 * math.pi / length)
    return jnp.concatenate(
        [jnp.cos(angles).astype(jnp.bfloat16), (-jnp.sin(angles)).astype(jnp.bfloat16)], axis=0
    )


def update(current, spectral, skip_matrix):
    shape_lead = current.shape
    direct = jnp.dot(
        current.reshape(-1, shape_lead[-1]), skip_matrix, preferred_element_type=jnp.float32
    ).reshape(shape_lead)
    pre_act = spectral.astype(jnp.float32) + direct
    return (current.astype(jnp.float32) + jax.nn.gelu(pre_act, approximate=False)).astype(
        jnp.bfloat16
    )


def per_device(field, mode_table, analysis, synthesis, mixing, degree_gain, skip_weight):
    xs = lax.axis_size("latx")
    cores = lax.axis_size("core")
    lons = lax.axis_size("lon")
    core = lax.axis_index("core")
    lat_dev, lon_dev, channels = field.shape
    points = lon_dev * lons
    degrees = analysis.shape[1]
    slots = analysis.shape[0]
    band = lat_dev // lons
    rows_full = lat_dev * xs * cores
    owners = xs * lons
    bf16 = jnp.bfloat16
    f32 = jnp.float32

    rows = lax.all_to_all(field, "lon", split_axis=0, concat_axis=1, tiled=True)

    orders = mode_table.reshape(xs, cores, lons, slots)
    flip = core == 1
    own_orders = jnp.where(flip, orders[:, 1], orders[:, 0]).reshape(-1)
    far_orders = jnp.where(flip, orders[:, 0], orders[:, 1]).reshape(-1)
    far_table = fourier_table(far_orders, points)
    own_table = fourier_table(own_orders, points)

    place = jnp.arange(rows_full, dtype=jnp.int32)
    place_row = place % band
    place_core = (place // band) % cores
    place_lon = (place // (band * cores)) % lons
    place_x = place // (band * cores * lons)
    real_core = jnp.where(flip, 1 - place_core, place_core)
    real_row = ((place_x * cores + real_core) * lons + place_lon) * band + place_row
    pick = (jnp.arange(rows_full, dtype=jnp.int32)[:, None] == real_row[None, :]).astype(bf16)

    def picked(table):
        return jnp.dot(
            table.reshape(slots * degrees, rows_full), pick, preferred_element_type=f32
        ).astype(bf16).reshape(slots, degrees, rows_full)

    far_side = jnp.einsum("qk,rkc->qrc", far_table, rows, preferred_element_type=f32).astype(bf16)
    far_in = lax.ppermute(far_side, "core", SWAP)
    own_side = jnp.einsum("qk,rkc->qrc", own_table, rows, preferred_element_type=f32).astype(bf16)
    both = jnp.concatenate([own_side, far_in], axis=1)
    both = both.reshape(2, owners, slots, cores * band, channels)
    both = jnp.transpose(both, (1, 0, 2, 3, 4))
    gathered = lax.all_to_all(both, OWNERS, split_axis=0, concat_axis=0, tiled=True)
    lat_data = jnp.transpose(gathered, (1, 2, 0, 3, 4)).reshape(2, slots, rows_full, channels)

    forward = picked(analysis)
    backward = picked(synthesis)

    def degrees_of(part):
        return jnp.einsum("slj,sjc->slc", forward, part, preferred_element_type=f32).astype(bf16)

    def rows_of(part):
        return jnp.einsum("slj,slc->sjc", backward, part, preferred_element_type=f32).astype(bf16)

    def times(part, matrix):
        return jnp.einsum("slc,cd->sld", part, matrix, preferred_element_type=f32)

    coef_real = degrees_of(lat_data[0])
    coef_imag = degrees_of(lat_data[1])
    real_map = mixing[0, 0]
    imag_map = mixing[0, 1]
    gain = degree_gain[0][None]
    mixed_real = ((times(coef_real, real_map) - times(coef_imag, imag_map)) * gain).astype(bf16)
    mixed_imag = ((times(coef_real, imag_map) + times(coef_imag, real_map)) * gain).astype(bf16)
    mixed = jnp.stack([mixed_real, mixed_imag], axis=2)
    synthesized = jnp.stack([rows_of(mixed_real), rows_of(mixed_imag)], axis=0)
    synthesized = synthesized.reshape(2, slots, owners, cores * band, channels)
    synthesized = jnp.transpose(synthesized, (2, 0, 1, 3, 4))
    returned = lax.all_to_all(synthesized, OWNERS, split_axis=0, concat_axis=0, tiled=True)
    returned = jnp.transpose(returned, (1, 0, 2, 3, 4)).reshape(-1, cores * band, channels)
    far_back = lax.ppermute(returned[:, band:], "core", SWAP)
    own_back = returned[:, :band]
    spectral = jnp.einsum(
        "qrc,qk->rkc",
        jnp.concatenate([own_back, far_back], axis=0),
        jnp.concatenate([own_table, far_table], axis=0),
        preferred_element_type=f32,
    ).astype(bf16)
    spectral = jnp.transpose(spectral.reshape(band, lons, lon_dev, channels), (1, 0, 2, 3))
    grid_part = lax.all_to_all(spectral, "lon", split_axis=0, concat_axis=0, tiled=True)
    grid_part = grid_part.reshape(field.shape)
    return (update(field, grid_part, skip_weight[0]), mixed)


def solution(mesh):
    names = ("member", "latx", "core", "lon")
    sizes = dict(mesh.shape)
    chips = Mesh(
        mesh.devices.reshape(sizes["member"], sizes["lat"] // 2, 2, sizes["lon"]), names
    )
    in_specs = (
        P(("member", "latx", "core"), "lon", None),
        P(),
        P(("latx", "core", "lon"), None, None),
        P(("latx", "core", "lon"), None, None),
        P(),
        P(),
        P(),
    )
    out_specs = (
        P(("member", "latx", "core"), "lon", None),
        P(("member", "latx", "core", "lon"), None, None, None),
    )
    return jax.shard_map(
        per_device, mesh=chips, in_specs=in_specs, out_specs=out_specs, check_vma=False
    )
```

```python
import math

import jax
import jax.numpy as jnp
from jax import lax
from jax.sharding import Mesh, PartitionSpec as P


SWAP = [(0, 1), (1, 0)]
OWNERS = ("latx", "lon")


def fourier_table(orders, length):
    owners, slots = orders.shape
    wave = jnp.stack([orders, orders], axis=1).reshape(-1)
    turn = jnp.arange(2 * owners * slots, dtype=jnp.int32) // slots % 2 * (length // 4)
    phases = (wave[:, None] * jnp.arange(length, dtype=jnp.int32)[None, :] + turn[:, None]) % length
    return jnp.cos(phases.astype(jnp.float32) * (2.0 * math.pi / length)).astype(jnp.bfloat16)


def update(current, spectral, skip_matrix):
    shape_lead = current.shape
    direct = jnp.dot(
        current.reshape(-1, shape_lead[-1]), skip_matrix, preferred_element_type=jnp.float32
    ).reshape(shape_lead)
    pre_act = spectral.astype(jnp.float32) + direct
    half = 0.5 * pre_act
    return (
        current.astype(jnp.float32) + (half + half * lax.erf(pre_act * math.sqrt(0.5)))
    ).astype(jnp.bfloat16)


def per_device(field, mode_table, analysis, synthesis, mixing, degree_gain, skip_weight):
    xs = lax.axis_size("latx")
    cores = lax.axis_size("core")
    lons = lax.axis_size("lon")
    core = lax.axis_index("core")
    lat_dev, lon_dev, channels = field.shape
    points = lon_dev * lons
    degrees = analysis.shape[1]
    slots = analysis.shape[0]
    band = lat_dev // lons
    rows_full = lat_dev * xs * cores
    owners = xs * lons
    bf16 = jnp.bfloat16
    f32 = jnp.float32

    rows = lax.all_to_all(field, "lon", split_axis=0, concat_axis=1, tiled=True)

    orders = mode_table.reshape(xs, cores, lons, slots)
    flip = core == 1
    own_orders = jnp.where(flip, orders[:, 1], orders[:, 0]).reshape(owners, slots)
    far_orders = jnp.where(flip, orders[:, 0], orders[:, 1]).reshape(owners, slots)
    far_table, own_table = lax.optimization_barrier(
        (fourier_table(far_orders, points), fourier_table(own_orders, points))
    )

    place = jnp.arange(rows_full, dtype=jnp.int32)
    place_row = place % band
    place_core = (place // band) % cores
    place_lon = (place // (band * cores)) % lons
    place_x = place // (band * cores * lons)
    real_core = jnp.where(flip, 1 - place_core, place_core)
    real_row = ((place_x * cores + real_core) * lons + place_lon) * band + place_row
    pick = (jnp.arange(rows_full, dtype=jnp.int32)[:, None] == real_row[None, :]).astype(bf16)

    def picked(table):
        return jnp.dot(
            table.reshape(slots * degrees, rows_full), pick, preferred_element_type=f32
        ).astype(bf16).reshape(slots, degrees, rows_full)

    far_side = jnp.einsum("qk,rkc->qrc", far_table, rows, preferred_element_type=f32).astype(bf16)
    far_in = lax.ppermute(far_side, "core", SWAP)
    own_side = jnp.einsum("qk,rkc->qrc", own_table, rows, preferred_element_type=f32).astype(bf16)
    both = jnp.concatenate([own_side, far_in], axis=1)
    both = both.reshape(owners, 2, slots, cores * band, channels)
    gathered = lax.all_to_all(both, OWNERS, split_axis=0, concat_axis=0, tiled=True)
    lat_data = jnp.transpose(gathered, (1, 2, 0, 3, 4)).reshape(2, slots, rows_full, channels)

    forward = picked(analysis)
    backward = picked(synthesis)

    def degrees_of(part):
        return jnp.einsum("slj,sjc->slc", forward, part, preferred_element_type=f32).astype(bf16)

    def rows_of(part):
        return jnp.einsum("slj,slc->sjc", backward, part, preferred_element_type=f32).astype(bf16)

    def times(part, matrix):
        return jnp.einsum("slc,cd->sld", part, matrix, preferred_element_type=f32)

    coef_real = degrees_of(lat_data[0])
    coef_imag = degrees_of(lat_data[1])
    real_map = mixing[0, 0]
    imag_map = mixing[0, 1]
    gain = degree_gain[0][None]
    mixed_real = ((times(coef_real, real_map) - times(coef_imag, imag_map)) * gain).astype(bf16)
    mixed_imag = ((times(coef_real, imag_map) + times(coef_imag, real_map)) * gain).astype(bf16)
    mixed = jnp.stack([mixed_real, mixed_imag], axis=2)
    synthesized = jnp.stack([rows_of(mixed_real), rows_of(mixed_imag)], axis=0)
    synthesized = synthesized.reshape(2, slots, owners, cores * band, channels)
    synthesized = jnp.transpose(synthesized, (2, 0, 1, 3, 4))
    returned = lax.all_to_all(synthesized, OWNERS, split_axis=0, concat_axis=0, tiled=True)
    returned = returned.reshape(-1, cores * band, channels)
    far_back = lax.ppermute(returned[:, band:], "core", SWAP)

    def points_of(part, table):
        return jnp.einsum("qrc,qk->rkc", part, table, preferred_element_type=f32)

    spectral = (
        points_of(returned[:, :band], own_table) + points_of(far_back, far_table)
    ).astype(bf16)
    spectral = jnp.transpose(spectral.reshape(band, lons, lon_dev, channels), (1, 0, 2, 3))

    lon = lax.axis_index("lon")
    advanced = jnp.zeros_like(field)
    arrivals = [(lon, lax.dynamic_index_in_dim(spectral, lon, 0, keepdims=False))]
    for shift in sorted(range(1, lons), key=lambda step: -min(step, lons - step)):
        target = lax.rem(lon + shift, lons)
        block = lax.dynamic_index_in_dim(spectral, target, 0, keepdims=False)
        block = lax.ppermute(block, "lon", [(i, (i + shift) % lons) for i in range(lons)])
        arrivals.append((lax.rem(lon + lons - shift, lons), block))
    for source, block in arrivals:
        start = (source * band, 0, 0)
        current = lax.dynamic_slice(field, start, block.shape)
        advanced = lax.dynamic_update_slice(
            advanced, update(current, block, skip_weight[0]), start
        )
    return (advanced, mixed)


def solution(mesh):
    names = ("member", "latx", "core", "lon")
    sizes = dict(mesh.shape)
    chips = Mesh(
        mesh.devices.reshape(sizes["member"], sizes["lat"] // 2, 2, sizes["lon"]), names
    )
    in_specs = (
        P(("member", "latx", "core"), "lon", None),
        P(),
        P(("latx", "core", "lon"), None, None),
        P(("latx", "core", "lon"), None, None),
        P(),
        P(),
        P(),
    )
    out_specs = (
        P(("member", "latx", "core"), "lon", None),
        P(("member", "latx", "core", "lon"), None, None, None),
    )
    return jax.shard_map(
        per_device, mesh=chips, in_specs=in_specs, out_specs=out_specs, check_vma=False
    )
```

```python
import math

import jax
import jax.numpy as jnp
from jax import lax
from jax.sharding import Mesh, PartitionSpec as P


SWAP = [(0, 1), (1, 0)]
OWNERS = ("latx", "lon")


def fourier_table(orders, length):
    owners, slots = orders.shape
    wave = jnp.stack([orders, orders], axis=1).reshape(-1)
    turn = jnp.arange(2 * owners * slots, dtype=jnp.int32) // slots % 2 * (length // 4)
    phases = wave[:, None] * jnp.arange(length, dtype=jnp.int32)[None, :] + turn[:, None]
    folded = jnp.abs(phases % length - length // 2) - length // 4
    angle = folded.astype(jnp.float32) * (2.0 * math.pi / length)
    square = angle * angle
    series = jnp.float32(1.0 / math.factorial(13))
    for power in (11, 9, 7, 5, 3, 1):
        sign = -1.0 if power % 4 == 3 else 1.0
        series = series * square + jnp.float32(sign / math.factorial(power))
    return (angle * series).astype(jnp.bfloat16)


def per_device(field, mode_table, analysis, synthesis, mixing, degree_gain, skip_weight):
    xs = lax.axis_size("latx")
    cores = lax.axis_size("core")
    lons = lax.axis_size("lon")
    core = lax.axis_index("core")
    lon = lax.axis_index("lon")
    lat_dev, lon_dev, channels = field.shape
    half = channels // 2
    points = lon_dev * lons
    degrees = analysis.shape[1]
    slots = analysis.shape[0]
    band = lat_dev // lons
    rows_full = lat_dev * xs * cores
    owners = xs * lons
    bf16 = jnp.bfloat16
    f32 = jnp.float32
    shifts = sorted(range(1, lons), key=lambda step: -min(step, lons - step))

    def sent(block, shift):
        return lax.ppermute(block, "lon", [(i, (i + shift) % lons) for i in range(lons)])

    def after(value, *earlier):
        return lax.optimization_barrier((value, *earlier))[0]

    first = lax.all_to_all(
        field[:, :, :half].reshape(lons, band, lon_dev, half), "lon", 0, 0, tiled=True
    )
    rows_a = jnp.transpose(first, (1, 0, 2, 3)).reshape(band, points, half)

    def grid_block(place):
        return lax.dynamic_slice(field, (place * band, 0, half), (band, lon_dev, half))

    arrived = [(lon, grid_block(lon))]
    for shift in shifts:
        block = grid_block(lax.rem(lon + shift, lons))
        block = sent(block, shift)
        arrived.append((lax.rem(lon + lons - shift, lons), block))

    orders = mode_table.reshape(xs, cores, lons, slots)
    flip = core == 1
    own_orders = jnp.where(flip, orders[:, 1], orders[:, 0]).reshape(owners, slots)
    far_orders = jnp.where(flip, orders[:, 0], orders[:, 1]).reshape(owners, slots)
    far_table, own_table = lax.optimization_barrier(
        (fourier_table(far_orders, points), fourier_table(own_orders, points))
    )

    place = jnp.arange(rows_full, dtype=jnp.int32)
    place_row = place % band
    place_core = (place // band) % cores
    place_lon = (place // (band * cores)) % lons
    place_x = place // (band * cores * lons)
    real_core = jnp.where(flip, 1 - place_core, place_core)
    real_row = ((place_x * cores + real_core) * lons + place_lon) * band + place_row
    pick = (jnp.arange(rows_full, dtype=jnp.int32)[:, None] == real_row[None, :]).astype(bf16)

    def picked(table):
        return jnp.dot(
            table.reshape(slots * degrees, rows_full), pick, preferred_element_type=f32
        ).astype(bf16).reshape(slots, degrees, rows_full)

    def waves_of(rows):
        far_side = jnp.einsum("qk,rkc->qrc", far_table, rows, preferred_element_type=f32)
        far_in = lax.ppermute(far_side.astype(bf16), "core", SWAP)
        own_side = jnp.einsum("qk,rkc->qrc", own_table, rows, preferred_element_type=f32)
        both = jnp.concatenate([own_side.astype(bf16), far_in], axis=1)
        return lax.optimization_barrier(both.reshape(owners, 2, slots, cores * band, half))

    def gathered(both):
        both = lax.all_to_all(both, OWNERS, 0, 0, tiled=True)
        both = jnp.concatenate([both[:, 0], both[:, 1]], axis=3)
        return jnp.transpose(both, (1, 0, 2, 3)).reshape(slots, rows_full, 2 * half)

    waves_a = waves_of(rows_a)
    rows_b = after(jnp.zeros((band, lons, lon_dev, half), bf16), waves_a)
    for source, block in arrived:
        rows_b = lax.dynamic_update_slice(rows_b, block[:, None], (0, source, 0, 0))
    waves_b = waves_of(rows_b.reshape(band, points, half))

    forward = picked(after(analysis, waves_b))
    backward = picked(after(synthesis, waves_b))

    def degrees_of(part):
        return jnp.einsum("slj,sjc->slc", forward, part, preferred_element_type=f32).astype(bf16)

    def rows_of(part):
        return jnp.einsum("slj,slc->sjc", backward, part, preferred_element_type=f32).astype(bf16)

    real_map, imag_map = mixing[0, 0], mixing[0, 1]
    cuts = [slice(side * half, (side + 1) * half) for side in range(2)]
    sums = 0.0
    for cut, both in zip(cuts, (waves_a, waves_b)):
        coefficients = degrees_of(gathered(both))
        real_rows = [t[cut, c] for c in cuts for t in (real_map, imag_map)]
        imag_rows = [t[cut, c] for c in cuts for t in (-imag_map, real_map)]
        joined = jnp.concatenate(
            [jnp.concatenate(real_rows, axis=1), jnp.concatenate(imag_rows, axis=1)], axis=0
        )
        sums = sums + jnp.dot(
            coefficients.reshape(-1, 2 * half), joined, preferred_element_type=f32
        ).reshape(slots, degrees, 2 * channels)
    gain = jnp.concatenate([degree_gain[0][:, c] for c in cuts for _ in range(2)], axis=1)
    mixed = lax.optimization_barrier((sums * gain[None]).astype(bf16))
    outs = []
    for side in range(2):
        synthesized = rows_of(mixed[:, :, side * channels : (side + 1) * channels])
        synthesized = synthesized.reshape(slots, owners, cores * band, channels)
        synthesized = jnp.stack([synthesized[..., :half], synthesized[..., half:]], axis=0)
        outs.append(jnp.transpose(synthesized, (2, 0, 1, 3, 4)))
    spectrum = jnp.transpose(mixed.reshape(slots, degrees, 2, 2, half), (0, 1, 3, 2, 4))
    spectrum = spectrum.reshape(slots, degrees, 2, channels)

    def points_of(part, table):
        return jnp.einsum("qrc,qk->rkc", part, table, preferred_element_type=f32)

    def spectral_of(returned):
        returned = returned.reshape(-1, cores * band, half)
        own_back, far_back = returned[:, :band], returned[:, band:]
        far_back = lax.ppermute(far_back, "core", SWAP)
        spectral = points_of(own_back, own_table) + points_of(far_back, far_table)
        spectral = spectral.astype(bf16).reshape(band, lons, lon_dev, half)
        return jnp.transpose(spectral, (1, 0, 2, 3))

    back_a = lax.all_to_all(outs[0], OWNERS, 0, 0, tiled=True)
    back_b = lax.all_to_all(outs[1], OWNERS, 0, 0, tiled=True)
    spectral_a = spectral_of(back_a)
    pieces = [(lon, lax.dynamic_index_in_dim(spectral_a, lon, 0, keepdims=False))]
    for shift in shifts:
        block = lax.dynamic_index_in_dim(
            spectral_a, lax.rem(lon + shift, lons), 0, keepdims=False
        )
        block = sent(block, shift)
        pieces.append((lax.rem(lon + lons - shift, lons), block))
    spectral_b = spectral_of(back_b)
    grid_b = lax.all_to_all(spectral_b, "lon", 0, 0, tiled=True)
    grid_a = jnp.zeros((lons, band, lon_dev, half), bf16)
    for source, block in pieces:
        grid_a = lax.dynamic_update_slice(grid_a, block[None], (source, 0, 0, 0))
    spectral = jnp.concatenate([grid_a, grid_b], axis=3).reshape(field.shape)
    direct = jnp.dot(
        field.reshape(-1, channels), skip_weight[0], preferred_element_type=f32
    ).reshape(field.shape)
    direct = lax.optimization_barrier(direct)
    pre_act = spectral.astype(f32) + direct
    lower = 0.5 * pre_act
    advanced = field.astype(f32) + (lower + lower * lax.erf(pre_act * math.sqrt(0.5)))
    return (advanced.astype(bf16), spectrum)


def solution(mesh):
    names = ("member", "latx", "core", "lon")
    sizes = dict(mesh.shape)
    chips = Mesh(
        mesh.devices.reshape(sizes["member"], sizes["lat"] // 2, 2, sizes["lon"]), names
    )
    in_specs = (
        P(("member", "latx", "core"), "lon", None),
        P(),
        P(("latx", "core", "lon"), None, None),
        P(("latx", "core", "lon"), None, None),
        P(),
        P(),
        P(),
    )
    out_specs = (
        P(("member", "latx", "core"), "lon", None),
        P(("member", "latx", "core", "lon"), None, None, None),
    )

    return jax.shard_map(
        per_device, mesh=chips, in_specs=in_specs, out_specs=out_specs, check_vma=False
    )
```

```python
import math

import jax
import jax.numpy as jnp
from jax import lax
from jax.experimental import pallas as pl
from jax.experimental.pallas import tpu as pltpu
from jax.sharding import Mesh, PartitionSpec as P


SWAP = [(0, 1), (1, 0)]
OWNERS = ("latx", "lon")


def fourier_table(orders, length):
    owners, slots = orders.shape
    wave = jnp.stack([orders, orders], axis=1).reshape(-1)
    turn = jnp.arange(2 * owners * slots, dtype=jnp.int32) // slots % 2 * (length // 4)
    phases = wave[:, None] * jnp.arange(length, dtype=jnp.int32)[None, :] + turn[:, None]
    folded = jnp.abs(phases % length - length // 2) - length // 4
    angle = folded.astype(jnp.float32) * (2.0 * math.pi / length)
    square = angle * angle
    series = jnp.float32(1.0 / math.factorial(13))
    for power in (11, 9, 7, 5, 3, 1):
        sign = -1.0 if power % 4 == 3 else 1.0
        series = series * square + jnp.float32(sign / math.factorial(power))
    return (angle * series).astype(jnp.bfloat16)


def update(current, spectral, skip_matrix):
    shape_lead = current.shape
    direct = jnp.dot(
        current.reshape(-1, shape_lead[-1]), skip_matrix, preferred_element_type=jnp.float32
    ).reshape(shape_lead)
    pre_act = spectral.astype(jnp.float32) + direct
    half = 0.5 * pre_act
    return (
        current.astype(jnp.float32) + (half + half * lax.erf(pre_act * math.sqrt(0.5)))
    ).astype(jnp.bfloat16)


def spectral_body(waves, forward, backward, mixing, gain, packed, mixed):
    f32, bf16 = jnp.float32, jnp.bfloat16
    owners, _, _, rows, channels = waves.shape

    def dot(left, right):
        return jnp.dot(left, right, preferred_element_type=f32)

    coefs = []
    for part in range(2):
        wave = waves[:, part, 0].astype(f32).reshape(owners * rows, channels).astype(bf16)
        coefs.append(dot(forward[0], wave).astype(bf16))
    real, imag = coefs
    outs = [
        (dot(real, mixing[0]) - dot(imag, mixing[1])) * gain[...],
        (dot(real, mixing[1]) + dot(imag, mixing[0])) * gain[...],
    ]
    for part in range(2):
        out = outs[part].astype(bf16)
        mixed[0, :, part * channels : (part + 1) * channels] = out
        rows_out = dot(backward[0], out)
        packed[:, part, 0] = rows_out.reshape(owners, rows, channels).astype(bf16)


def spectral_step(waves, forward, backward, mixing, gain):
    owners, parts, slots, rows, channels = waves.shape
    degrees = forward.shape[1]
    wave_spec = pl.BlockSpec((owners, parts, 1, rows, channels), lambda s: (0, 0, s, 0, 0))
    return pl.pallas_call(
        spectral_body,
        grid=(slots,),
        in_specs=[
            wave_spec,
            pl.BlockSpec((1, degrees, owners * rows), lambda s: (s, 0, 0)),
            pl.BlockSpec((1, owners * rows, degrees), lambda s: (s, 0, 0)),
            pl.BlockSpec(mixing.shape, lambda s: (0, 0, 0)),
            pl.BlockSpec(gain.shape, lambda s: (0, 0)),
        ],
        out_specs=[
            wave_spec,
            pl.BlockSpec((1, degrees, parts * channels), lambda s: (s, 0, 0)),
        ],
        out_shape=[
            jax.ShapeDtypeStruct(waves.shape, waves.dtype),
            jax.ShapeDtypeStruct((slots, degrees, parts * channels), waves.dtype),
        ],
        cost_estimate=pl.CostEstimate(
            flops=4 * 10**9, bytes_accessed=10**7, transcendentals=0
        ),
    )(waves, forward, backward, mixing, gain)


def per_device(field, mode_table, analysis, synthesis, mixing, degree_gain, skip_weight):
    xs = lax.axis_size("latx")
    cores = lax.axis_size("core")
    lons = lax.axis_size("lon")
    core = lax.axis_index("core")
    lat_dev, lon_dev, channels = field.shape
    points = lon_dev * lons
    degrees = analysis.shape[1]
    slots = analysis.shape[0]
    band = lat_dev // lons
    rows_full = lat_dev * xs * cores
    owners = xs * lons
    bf16 = jnp.bfloat16
    f32 = jnp.float32

    def after(value, *earlier):
        return lax.optimization_barrier((value, *earlier))[0]

    blocks = lax.all_to_all(field, "lon", split_axis=0, concat_axis=0, tiled=True)

    orders = mode_table.reshape(xs, cores, lons, slots)
    flip = core == 1
    own_orders = jnp.where(flip, orders[:, 1], orders[:, 0]).reshape(owners, slots)
    far_orders = jnp.where(flip, orders[:, 0], orders[:, 1]).reshape(owners, slots)

    place = jnp.arange(rows_full, dtype=jnp.int32)
    place_row = place % band
    place_core = (place // band) % cores
    place_lon = (place // (band * cores)) % lons
    place_x = place // (band * cores * lons)
    real_core = jnp.where(flip, 1 - place_core, place_core)
    real_row = ((place_x * cores + real_core) * lons + place_lon) * band + place_row
    pick = (jnp.arange(rows_full, dtype=jnp.int32)[:, None] == real_row[None, :]).astype(bf16)

    forward = jnp.einsum("slj,jk->slk", analysis, pick, preferred_element_type=f32)
    backward = jnp.einsum("slj,jk->skl", synthesis, pick, preferred_element_type=f32)

    blocks, far_table, own_table, forward, backward = lax.optimization_barrier(
        (
            blocks,
            fourier_table(far_orders, points),
            fourier_table(own_orders, points),
            forward.astype(bf16),
            backward.astype(bf16),
        )
    )
    rows = jnp.transpose(blocks.reshape(lons, band, lon_dev, channels), (1, 0, 2, 3))
    rows = rows.reshape(band, points, channels)
    far_side = jnp.einsum("qk,rkc->qrc", far_table, rows, preferred_element_type=f32).astype(bf16)
    far_in = lax.ppermute(far_side, "core", SWAP)
    own_side = jnp.einsum("qk,rkc->qrc", own_table, rows, preferred_element_type=f32).astype(bf16)
    both = jnp.concatenate([own_side, far_in], axis=1)
    both = both.reshape(owners, -1, channels)
    gathered = lax.all_to_all(both, OWNERS, split_axis=0, concat_axis=0, tiled=True)
    packed, mixed = spectral_step(
        gathered.reshape(owners, 2, slots, cores * band, channels),
        forward,
        backward,
        mixing[0],
        degree_gain[0],
    )
    packed = packed.reshape(owners, -1, channels)
    returned = lax.all_to_all(packed, OWNERS, split_axis=0, concat_axis=0, tiled=True)
    spectrum = mixed.reshape(slots, degrees, 2, channels)
    returned = returned.reshape(-1, cores * band, channels)
    far_back = lax.ppermute(returned[:, band:], "core", SWAP)

    def points_of(part, table):
        return jnp.einsum("qrc,qk->rkc", part, table, preferred_element_type=f32)

    spectral = (
        points_of(returned[:, :band], own_table) + points_of(far_back, far_table)
    ).astype(bf16)
    spectral = jnp.transpose(spectral.reshape(band, lons, lon_dev, channels), (1, 0, 2, 3))

    lon = lax.axis_index("lon")
    advanced = jnp.zeros_like(field)
    arrivals = [(lon, lax.dynamic_index_in_dim(spectral, lon, 0, keepdims=False))]
    for shift in sorted(range(1, lons), key=lambda step: -min(step, lons - step)):
        target = lax.rem(lon + shift, lons)
        block = lax.dynamic_index_in_dim(spectral, target, 0, keepdims=False)
        block = lax.ppermute(block, "lon", [(i, (i + shift) % lons) for i in range(lons)])
        arrivals.append((lax.rem(lon + lons - shift, lons), block))
    for source, block in arrivals:
        start = (source * band, 0, 0)
        current = lax.dynamic_slice(field, start, block.shape)
        weight = after(skip_weight[0], block)
        advanced = lax.dynamic_update_slice(advanced, update(current, block, weight), start)
    return (advanced, spectrum)


def solution(mesh):
    names = ("member", "latx", "core", "lon")
    sizes = dict(mesh.shape)
    chips = Mesh(
        mesh.devices.reshape(sizes["member"], sizes["lat"] // 2, 2, sizes["lon"]), names
    )
    in_specs = (
        P(("member", "latx", "core"), "lon", None),
        P(),
        P(("latx", "core", "lon"), None, None),
        P(("latx", "core", "lon"), None, None),
        P(),
        P(),
        P(),
    )
    out_specs = (
        P(("member", "latx", "core"), "lon", None),
        P(("member", "latx", "core", "lon"), None, None, None),
    )
    return jax.shard_map(
        per_device, mesh=chips, in_specs=in_specs, out_specs=out_specs, check_vma=False
    )
```

```python
import math

import jax
import jax.numpy as jnp
from jax import lax
from jax.experimental import pallas as pl
from jax.experimental.pallas import tpu as pltpu
from jax.sharding import Mesh, PartitionSpec as P


SWAP = [(0, 1), (1, 0)]
OWNERS = ("latx", "lon")
HOLD_FIRST = 8
HOLD_THIRD = 16


def fourier_table(orders, length, turn):
    phases = orders[:, None] * jnp.arange(length, dtype=jnp.int32)[None, :] + turn
    folded = jnp.abs(phases % length - length // 2) - length // 4
    angle = folded.astype(jnp.float32) * (2.0 * math.pi / length)
    square = angle * angle
    series = jnp.float32(1.0 / math.factorial(13))
    for power in (11, 9, 7, 5, 3, 1):
        sign = -1.0 if power % 4 == 3 else 1.0
        series = series * square + jnp.float32(sign / math.factorial(power))
    return (angle * series).astype(jnp.bfloat16)


def spectral_body(own, far, forward, backward, mixing, gain, own_out, far_out, mixed):
    f32, bf16 = jnp.float32, jnp.bfloat16
    owners, _, _, rows, channels = own.shape
    count = owners * rows // 2
    band = rows // 2
    lower = lax.broadcasted_iota(jnp.int32, (owners // 2, rows, channels), 1) < band

    def dot(left, right):
        return jnp.dot(left, right, preferred_element_type=f32)

    def turned(tiles):
        return pltpu.roll(tiles, band, 1)

    def parted(first, second):
        return jnp.where(lower, first, turned(second)), jnp.where(lower, turned(first), second)

    waves = []
    for wave in (own[:, 0, 0], far[:, 0]):
        wave = wave.astype(f32)
        parts = parted(wave[: owners // 2], wave[owners // 2 :])
        waves.append([part.reshape(count, channels).astype(bf16) for part in parts])
    coefs = []
    for part in range(2):
        total = dot(forward[0, :, :count], waves[0][part])
        coefs.append((total + dot(forward[0, :, count:], waves[1][part])).astype(bf16))
    real, imag = coefs
    outs = [
        (dot(real, mixing[0]) - dot(imag, mixing[1])) * gain[...],
        (dot(real, mixing[1]) + dot(imag, mixing[0])) * gain[...],
    ]
    outs = [out.astype(bf16) for out in outs]
    for part in range(2):
        mixed[0, :, part * channels : (part + 1) * channels] = outs[part]
    for side, target in enumerate((own_out, far_out)):
        table = backward[0, side * count : (side + 1) * count, :]
        tiles = [dot(table, out).reshape(owners // 2, rows, channels) for out in outs]
        first, second = parted(*tiles)
        target[: owners // 2, 0] = first.astype(bf16)
        target[owners // 2 :, 0] = second.astype(bf16)


def spectral_step(waves, far, forward, backward, mixing, gain):
    owners, _, slots, rows, channels = waves.shape
    degrees = forward.shape[1]
    far_spec = pl.BlockSpec((owners, 1, rows, channels), lambda s: (0, s, 0, 0))
    return pl.pallas_call(
        spectral_body,
        grid=(slots,),
        in_specs=[
            pl.BlockSpec((owners, 1, 1, rows, channels), lambda s: (0, 0, s, 0, 0)),
            far_spec,
            pl.BlockSpec((1, *forward.shape[1:]), lambda s: (s, 0, 0)),
            pl.BlockSpec((1, *backward.shape[1:]), lambda s: (s, 0, 0)),
            pl.BlockSpec(mixing.shape, lambda s: (0, 0, 0)),
            pl.BlockSpec(gain.shape, lambda s: (0, 0)),
        ],
        out_specs=[
            far_spec,
            far_spec,
            pl.BlockSpec((1, degrees, 2 * channels), lambda s: (s, 0, 0)),
        ],
        out_shape=[
            jax.ShapeDtypeStruct(far.shape, far.dtype),
            jax.ShapeDtypeStruct(far.shape, far.dtype),
            jax.ShapeDtypeStruct((slots, degrees, 2 * channels), far.dtype),
        ],
        cost_estimate=pl.CostEstimate(
            flops=4 * 10**9, bytes_accessed=10**7, transcendentals=0
        ),
    )(waves, far, forward, backward, mixing, gain)


def per_device(field, mode_table, analysis, synthesis, mixing, degree_gain, skip_weight):
    xs = lax.axis_size("latx")
    cores = lax.axis_size("core")
    lons = lax.axis_size("lon")
    core = lax.axis_index("core")
    lat_dev, lon_dev, channels = field.shape
    points = lon_dev * lons
    degrees = analysis.shape[1]
    slots = analysis.shape[0]
    band = lat_dev // lons
    rows_full = lat_dev * xs * cores
    owners = xs * lons
    bf16 = jnp.bfloat16
    f32 = jnp.float32
    flip = core == 1

    def spent(turns, level):
        def turn(_, state):
            held, flag = state
            held = jnp.abs(jnp.dot(held, held, preferred_element_type=f32)).astype(bf16)
            return held, flag | (held[0, 0] < 0)

        start = jnp.full((256, 256), level, bf16)
        return lax.fori_loop(0, jnp.where(flip, 0, turns), turn, (start, False))[1]

    def everywhere(value):
        return lax.all_to_all(value, OWNERS, split_axis=0, concat_axis=0, tiled=True)

    flag = spent(HOLD_FIRST, 1e-2)
    blocks = lax.all_to_all(field, "lon", split_axis=0, concat_axis=0, tiled=True)

    orders = jnp.transpose(mode_table.reshape(xs, cores, lons, slots), (0, 2, 1, 3))
    orders = jnp.where(flip, orders[:, :, ::-1], orders).reshape(-1)

    place = jnp.arange(rows_full, dtype=jnp.int32)
    place_row = place % band
    place_chip = place // (2 * band) % (owners // 2) + place // band % 2 * (owners // 2)
    place_side = place // (band * owners)
    place_core = jnp.where(flip, 1 - place_side, place_side)
    real_row = ((place_chip // lons * cores + place_core) * lons + place_chip % lons) * band
    real_row = real_row + place_row
    pick = (jnp.arange(rows_full, dtype=jnp.int32)[:, None] == real_row[None, :]).astype(bf16)
    forward = jnp.einsum("slj,jk->slk", analysis, pick, preferred_element_type=f32)
    backward = jnp.einsum("slj,jk->skl", synthesis, pick, preferred_element_type=f32)

    blocks, real_table, imag_table, forward, backward = lax.optimization_barrier(
        (
            blocks,
            fourier_table(orders, points, 0),
            fourier_table(orders, points, points // 4),
            forward.astype(bf16),
            backward.astype(bf16),
        )
    )
    rows = jnp.transpose(blocks.reshape(lons, band, lon_dev, channels), (1, 0, 2, 3))
    rows = rows.reshape(band, points, channels)

    def waves_of(table):
        return jnp.einsum("qk,rkc->qrc", table, rows, preferred_element_type=f32).astype(bf16)

    both = jnp.concatenate([waves_of(real_table), waves_of(imag_table)], axis=1)
    waves = everywhere(both.reshape(owners, -1, channels))
    waves = waves.reshape(owners, cores, slots, 2 * band, channels)
    far = lax.ppermute(waves[:, 1], "core", SWAP)
    own_out, far_out, mixed = spectral_step(
        waves, far, forward, backward, mixing[0], degree_gain[0]
    )
    far_back = lax.ppermute(far_out, "core", SWAP)
    flag = flag | spent(HOLD_THIRD, 2e-2)
    packed = jnp.stack([own_out, far_back], axis=1).reshape(owners, -1, channels)
    packed = jnp.where(flag, jnp.zeros_like(packed), packed)
    returned = everywhere(packed).reshape(-1, 2 * band, channels)

    def points_of(part, table):
        return jnp.einsum("qrc,qk->rkc", part, table, preferred_element_type=f32)

    spectral = (
        points_of(returned[:, :band], real_table) + points_of(returned[:, band:], imag_table)
    ).astype(bf16)
    spectral = jnp.transpose(spectral.reshape(band, lons, lon_dev, channels), (1, 0, 2, 3))
    spectral = lax.all_to_all(
        spectral.reshape(lat_dev, lon_dev, channels), "lon", 0, 0, tiled=True
    )
    direct = jnp.dot(
        field.reshape(-1, channels), skip_weight[0], preferred_element_type=f32
    ).reshape(field.shape)
    direct = lax.optimization_barrier(direct)
    pre_act = spectral.astype(f32) + direct
    half = 0.5 * pre_act
    advanced = field.astype(f32) + (half + half * lax.erf(pre_act * math.sqrt(0.5)))
    return (advanced.astype(bf16), mixed.reshape(slots, degrees, 2, channels))


def solution(mesh):
    names = ("member", "latx", "core", "lon")
    sizes = dict(mesh.shape)
    chips = Mesh(
        mesh.devices.reshape(sizes["member"], sizes["lat"] // 2, 2, sizes["lon"]), names
    )
    in_specs = (
        P(("member", "latx", "core"), "lon", None),
        P(),
        P(("latx", "core", "lon"), None, None),
        P(("latx", "core", "lon"), None, None),
        P(),
        P(),
        P(),
    )
    out_specs = (
        P(("member", "latx", "core"), "lon", None),
        P(("member", "latx", "core", "lon"), None, None, None),
    )

    return jax.shard_map(
        per_device, mesh=chips, in_specs=in_specs, out_specs=out_specs, check_vma=False
    )
```

```python
import math

import jax
import jax.numpy as jnp
from jax import lax
from jax.experimental import pallas as pl
from jax.experimental.pallas import tpu as pltpu
from jax.sharding import Mesh, PartitionSpec as P


SWAP = [(0, 1), (1, 0)]
OWNERS = ("latx", "lon")
HOLD_FIRST = 10
HOLD_THIRD = 16


def fourier_table(orders, length, turn):
    phases = orders[:, None] * jnp.arange(length, dtype=jnp.int32)[None, :] + turn
    folded = jnp.abs(phases % length - length // 2) - length // 4
    angle = folded.astype(jnp.float32) * (2.0 * math.pi / length)
    square = angle * angle
    series = jnp.float32(1.0 / math.factorial(13))
    for power in (11, 9, 7, 5, 3, 1):
        sign = -1.0 if power % 4 == 3 else 1.0
        series = series * square + jnp.float32(sign / math.factorial(power))
    return (angle * series).astype(jnp.bfloat16)


def spectral_body(own, far, forward, backward, mixing, gain, own_out, far_out, mixed):
    f32, bf16 = jnp.float32, jnp.bfloat16
    owners, _, _, rows, channels = own.shape
    count = owners * rows // 2
    band = rows // 2
    lower = lax.broadcasted_iota(jnp.int32, (owners // 2, rows, channels), 1) < band

    def dot(left, right):
        return jnp.dot(left, right, preferred_element_type=f32)

    def turned(tiles):
        return pltpu.roll(tiles, band, 1)

    def parted(first, second):
        return jnp.where(lower, first, turned(second)), jnp.where(lower, turned(first), second)

    waves = []
    for wave in (own[:, 0, 0], far[:, 0]):
        wave = wave.astype(f32)
        parts = parted(wave[: owners // 2], wave[owners // 2 :])
        waves.append([part.reshape(count, channels).astype(bf16) for part in parts])
    coefs = []
    for part in range(2):
        total = dot(forward[0, :, :count], waves[0][part])
        coefs.append((total + dot(forward[0, :, count:], waves[1][part])).astype(bf16))
    real, imag = coefs
    outs = [
        (dot(real, mixing[0]) - dot(imag, mixing[1])) * gain[...],
        (dot(real, mixing[1]) + dot(imag, mixing[0])) * gain[...],
    ]
    outs = [out.astype(bf16) for out in outs]
    for part in range(2):
        mixed[0, :, part * channels : (part + 1) * channels] = outs[part]
    for side in range(2):
        table = backward[0, side * count : (side + 1) * count, :]
        tiles = [dot(table, out).reshape(owners // 2, rows, channels) for out in outs]
        first, second = parted(*tiles)
        if side == 0:
            own_out[: owners // 2, 0, 0] = first.astype(bf16)
            own_out[owners // 2 :, 0, 0] = second.astype(bf16)
        else:
            far_out[: owners // 2, 0] = first.astype(bf16)
            far_out[owners // 2 :, 0] = second.astype(bf16)


def spectral_step(waves, far, forward, backward, mixing, gain):
    owners, _, slots, rows, channels = waves.shape
    degrees = forward.shape[1]
    own_spec = pl.BlockSpec((owners, 1, 1, rows, channels), lambda s: (0, 0, s, 0, 0))
    far_spec = pl.BlockSpec((owners, 1, rows, channels), lambda s: (0, s, 0, 0))
    return pl.pallas_call(
        spectral_body,
        grid=(slots,),
        in_specs=[
            own_spec,
            far_spec,
            pl.BlockSpec((1, *forward.shape[1:]), lambda s: (s, 0, 0)),
            pl.BlockSpec((1, *backward.shape[1:]), lambda s: (s, 0, 0)),
            pl.BlockSpec(mixing.shape, lambda s: (0, 0, 0)),
            pl.BlockSpec(gain.shape, lambda s: (0, 0)),
        ],
        out_specs=[
            own_spec,
            far_spec,
            pl.BlockSpec((1, degrees, 2 * channels), lambda s: (s, 0, 0)),
        ],
        out_shape=[
            jax.ShapeDtypeStruct(waves.shape, waves.dtype),
            jax.ShapeDtypeStruct(far.shape, far.dtype),
            jax.ShapeDtypeStruct((slots, degrees, 2 * channels), far.dtype),
        ],
        cost_estimate=pl.CostEstimate(
            flops=4 * 10**9, bytes_accessed=10**7, transcendentals=0
        ),
    )(waves, far, forward, backward, mixing, gain)


def per_device(field, mode_table, analysis, synthesis, mixing, degree_gain, skip_weight):
    xs = lax.axis_size("latx")
    cores = lax.axis_size("core")
    lons = lax.axis_size("lon")
    core = lax.axis_index("core")
    lat_dev, lon_dev, channels = field.shape
    points = lon_dev * lons
    degrees = analysis.shape[1]
    slots = analysis.shape[0]
    band = lat_dev // lons
    rows_full = lat_dev * xs * cores
    owners = xs * lons
    bf16 = jnp.bfloat16
    f32 = jnp.float32
    flip = core == 1

    def spent(turns, level):
        def turn(_, state):
            held, flag = state
            held = jnp.abs(jnp.dot(held, held, preferred_element_type=f32)).astype(bf16)
            return held, flag | (held[0, 0] < 0)

        start = jnp.full((256, 256), level, bf16)
        return lax.fori_loop(0, jnp.where(flip, 0, turns), turn, (start, False))[1]

    def everywhere(value):
        return lax.all_to_all(value, OWNERS, split_axis=0, concat_axis=0, tiled=True)

    flag = spent(HOLD_FIRST, 1e-2)
    blocks = lax.all_to_all(field, "lon", split_axis=0, concat_axis=0, tiled=True)

    orders = jnp.transpose(mode_table.reshape(xs, cores, lons, slots), (0, 2, 1, 3))
    orders = jnp.where(flip, orders[:, :, ::-1], orders).reshape(-1)

    place = jnp.arange(rows_full, dtype=jnp.int32)
    place_row = place % band
    place_chip = place // (2 * band) % (owners // 2) + place // band % 2 * (owners // 2)
    place_side = place // (band * owners)
    place_core = jnp.where(flip, 1 - place_side, place_side)
    real_row = ((place_chip // lons * cores + place_core) * lons + place_chip % lons) * band
    real_row = real_row + place_row
    pick = (jnp.arange(rows_full, dtype=jnp.int32)[:, None] == real_row[None, :]).astype(bf16)
    forward = jnp.einsum("slj,jk->slk", analysis, pick, preferred_element_type=f32)
    backward = jnp.einsum("slj,jk->skl", synthesis, pick, preferred_element_type=f32)

    blocks, real_table, imag_table, forward, backward = lax.optimization_barrier(
        (
            blocks,
            fourier_table(orders, points, 0),
            fourier_table(orders, points, points // 4),
            forward.astype(bf16),
            backward.astype(bf16),
        )
    )
    rows = jnp.transpose(blocks.reshape(lons, band, lon_dev, channels), (1, 0, 2, 3))
    rows = rows.reshape(band, points, channels)

    def waves_of(table):
        return jnp.einsum("qk,rkc->qrc", table, rows, preferred_element_type=f32).astype(bf16)

    both = jnp.concatenate([waves_of(real_table), waves_of(imag_table)], axis=1)
    waves = everywhere(both.reshape(owners, -1, channels))
    waves = waves.reshape(owners, cores, slots, 2 * band, channels)
    far = lax.ppermute(waves[:, 1], "core", SWAP)
    own_out, far_out, mixed = spectral_step(
        waves, far, forward, backward, mixing[0], degree_gain[0]
    )
    far_back = lax.ppermute(far_out, "core", SWAP)
    flag = flag | spent(HOLD_THIRD, 2e-2)
    far_back = jnp.where(flag, jnp.zeros_like(far_back), far_back)
    packed = lax.dynamic_update_slice(own_out, far_back[:, None], (0, 1, 0, 0, 0))
    packed = packed.reshape(owners, -1, channels)
    returned = everywhere(packed).reshape(-1, 2 * band, channels)

    def points_of(part, table):
        return jnp.einsum("qrc,qk->rkc", part, table, preferred_element_type=f32)

    spectral = (
        points_of(returned[:, :band], real_table) + points_of(returned[:, band:], imag_table)
    ).astype(bf16)
    spectral = jnp.transpose(spectral.reshape(band, lons, lon_dev, channels), (1, 0, 2, 3))
    spectral = lax.all_to_all(
        spectral.reshape(lat_dev, lon_dev, channels), "lon", 0, 0, tiled=True
    )
    direct = jnp.dot(
        field.reshape(-1, channels), skip_weight[0], preferred_element_type=f32
    ).reshape(field.shape)
    direct = lax.optimization_barrier(direct)
    pre_act = spectral.astype(f32) + direct
    half = 0.5 * pre_act
    advanced = field.astype(f32) + (half + half * lax.erf(pre_act * math.sqrt(0.5)))
    return (advanced.astype(bf16), mixed.reshape(slots, degrees, 2, channels))


def solution(mesh):
    names = ("member", "latx", "core", "lon")
    sizes = dict(mesh.shape)
    chips = Mesh(
        mesh.devices.reshape(sizes["member"], sizes["lat"] // 2, 2, sizes["lon"]), names
    )
    in_specs = (
        P(("member", "latx", "core"), "lon", None),
        P(),
        P(("latx", "core", "lon"), None, None),
        P(("latx", "core", "lon"), None, None),
        P(),
        P(),
        P(),
    )
    out_specs = (
        P(("member", "latx", "core"), "lon", None),
        P(("member", "latx", "core", "lon"), None, None, None),
    )

    return jax.shard_map(
        per_device, mesh=chips, in_specs=in_specs, out_specs=out_specs, check_vma=False
    )
```

```python
import math

import jax
import jax.numpy as jnp
from jax import lax
from jax.experimental import pallas as pl
from jax.experimental.pallas import tpu as pltpu
from jax.sharding import Mesh, PartitionSpec as P


SWAP = [(0, 1), (1, 0)]
OWNERS = ("latx", "lon")
HOLD_FIRST = 11
HOLD_THIRD = 15


def fourier_table(orders, length, turn):
    phases = orders[:, None] * jnp.arange(length, dtype=jnp.int32)[None, :] + turn
    folded = jnp.abs(phases % length - length // 2) - length // 4
    angle = folded.astype(jnp.float32) * (2.0 * math.pi / length)
    square = angle * angle
    series = jnp.float32(1.0 / math.factorial(13))
    for power in (11, 9, 7, 5, 3, 1):
        sign = -1.0 if power % 4 == 3 else 1.0
        series = series * square + jnp.float32(sign / math.factorial(power))
    return (angle * series).astype(jnp.bfloat16)


def spectral_body(own, far, forward, backward, mixing, gain, own_out, far_out, mixed):
    f32, bf16 = jnp.float32, jnp.bfloat16
    owners, _, _, rows, channels = own.shape
    count = owners * rows // 2
    band = rows // 2
    lower = lax.broadcasted_iota(jnp.int32, (owners // 2, rows, channels), 1) < band

    def dot(left, right):
        return jnp.dot(left, right, preferred_element_type=f32)

    def turned(tiles):
        return pltpu.roll(tiles, band, 1)

    def parted(first, second):
        return jnp.where(lower, first, turned(second)), jnp.where(lower, turned(first), second)

    waves = []
    for wave in (own[:, 0, 0], far[:, 0]):
        wave = wave.astype(f32)
        parts = parted(wave[: owners // 2], wave[owners // 2 :])
        waves.append([part.reshape(count, channels).astype(bf16) for part in parts])
    coefs = []
    for part in range(2):
        total = dot(forward[0, :, :count], waves[0][part])
        coefs.append((total + dot(forward[0, :, count:], waves[1][part])).astype(bf16))
    real, imag = coefs
    outs = [
        (dot(real, mixing[0]) - dot(imag, mixing[1])) * gain[...],
        (dot(real, mixing[1]) + dot(imag, mixing[0])) * gain[...],
    ]
    outs = [out.astype(bf16) for out in outs]
    for part in range(2):
        mixed[0, :, part * channels : (part + 1) * channels] = outs[part]
    for side in range(2):
        table = backward[0, side * count : (side + 1) * count, :]
        tiles = [dot(table, out).reshape(owners // 2, rows, channels) for out in outs]
        first, second = parted(*tiles)
        if side == 0:
            own_out[: owners // 2, 0, 0] = first.astype(bf16)
            own_out[owners // 2 :, 0, 0] = second.astype(bf16)
        else:
            far_out[: owners // 2, 0] = first.astype(bf16)
            far_out[owners // 2 :, 0] = second.astype(bf16)


def spectral_step(waves, far, forward, backward, mixing, gain):
    owners, _, slots, rows, channels = waves.shape
    degrees = forward.shape[1]
    own_spec = pl.BlockSpec((owners, 1, 1, rows, channels), lambda s: (0, 0, s, 0, 0))
    far_spec = pl.BlockSpec((owners, 1, rows, channels), lambda s: (0, s, 0, 0))
    return pl.pallas_call(
        spectral_body,
        grid=(slots,),
        in_specs=[
            own_spec,
            far_spec,
            pl.BlockSpec((1, *forward.shape[1:]), lambda s: (s, 0, 0)),
            pl.BlockSpec((1, *backward.shape[1:]), lambda s: (s, 0, 0)),
            pl.BlockSpec(mixing.shape, lambda s: (0, 0, 0)),
            pl.BlockSpec(gain.shape, lambda s: (0, 0)),
        ],
        out_specs=[
            own_spec,
            far_spec,
            pl.BlockSpec((1, degrees, 2 * channels), lambda s: (s, 0, 0)),
        ],
        out_shape=[
            jax.ShapeDtypeStruct(waves.shape, waves.dtype),
            jax.ShapeDtypeStruct(far.shape, far.dtype),
            jax.ShapeDtypeStruct((slots, degrees, 2 * channels), far.dtype),
        ],
        cost_estimate=pl.CostEstimate(
            flops=4 * 10**9, bytes_accessed=10**7, transcendentals=0
        ),
    )(waves, far, forward, backward, mixing, gain)


def per_device(field, mode_table, analysis, synthesis, mixing, degree_gain, skip_weight):
    xs = lax.axis_size("latx")
    cores = lax.axis_size("core")
    lons = lax.axis_size("lon")
    core = lax.axis_index("core")
    lat_dev, lon_dev, channels = field.shape
    points = lon_dev * lons
    degrees = analysis.shape[1]
    slots = analysis.shape[0]
    band = lat_dev // lons
    rows_full = lat_dev * xs * cores
    owners = xs * lons
    bf16 = jnp.bfloat16
    f32 = jnp.float32
    flip = core == 1

    def spent(turns, level):
        def turn(_, state):
            held, flag = state
            held = jnp.abs(jnp.dot(held, held, preferred_element_type=f32)).astype(bf16)
            return held, flag | (held[0, 0] < 0)

        start = jnp.full((256, 256), level, bf16)
        return lax.fori_loop(0, jnp.where(flip, 0, turns), turn, (start, False))[1]

    def everywhere(value):
        return lax.all_to_all(value, OWNERS, split_axis=0, concat_axis=0, tiled=True)

    flag = spent(HOLD_FIRST, 1e-2)
    blocks = lax.all_to_all(field, "lon", split_axis=0, concat_axis=0, tiled=True)

    orders = jnp.transpose(mode_table.reshape(xs, cores, lons, slots), (0, 2, 1, 3))
    orders = jnp.where(flip, orders[:, :, ::-1], orders).reshape(-1)

    place = jnp.arange(rows_full, dtype=jnp.int32)
    place_row = place % band
    place_chip = place // (2 * band) % (owners // 2) + place // band % 2 * (owners // 2)
    place_side = place // (band * owners)
    place_core = jnp.where(flip, 1 - place_side, place_side)
    real_row = ((place_chip // lons * cores + place_core) * lons + place_chip % lons) * band
    real_row = real_row + place_row
    pick = (jnp.arange(rows_full, dtype=jnp.int32)[:, None] == real_row[None, :]).astype(bf16)
    forward = jnp.einsum("slj,jk->slk", analysis, pick, preferred_element_type=f32)
    backward = jnp.einsum("slj,jk->skl", synthesis, pick, preferred_element_type=f32)

    blocks, real_table, imag_table, forward, backward = lax.optimization_barrier(
        (
            blocks,
            fourier_table(orders, points, 0),
            fourier_table(orders, points, points // 4),
            forward.astype(bf16),
            backward.astype(bf16),
        )
    )
    rows = jnp.transpose(blocks.reshape(lons, band, lon_dev, channels), (1, 0, 2, 3))
    rows = rows.reshape(band, points, channels)

    def waves_of(table):
        return jnp.einsum("qk,rkc->qrc", table, rows, preferred_element_type=f32).astype(bf16)

    both = jnp.concatenate([waves_of(real_table), waves_of(imag_table)], axis=1)
    waves = everywhere(both.reshape(owners, -1, channels))
    waves = waves.reshape(owners, cores, slots, 2 * band, channels)
    far = lax.ppermute(waves[:, 1], "core", SWAP)
    own_out, far_out, mixed = spectral_step(
        waves, far, forward, backward, mixing[0], degree_gain[0]
    )
    far_back = lax.ppermute(far_out, "core", SWAP)
    flag = flag | spent(HOLD_THIRD, 2e-2)
    far_back = jnp.where(flag, jnp.zeros_like(far_back), far_back)
    packed = lax.dynamic_update_slice(own_out, far_back[:, None], (0, 1, 0, 0, 0))
    packed = packed.reshape(owners, -1, channels)
    returned = everywhere(packed).reshape(-1, 2 * band, channels)

    def points_of(part, table):
        return jnp.einsum("qrc,qk->rkc", part, table, preferred_element_type=f32)

    spectral = (
        points_of(returned[:, :band], real_table) + points_of(returned[:, band:], imag_table)
    ).astype(bf16)
    spectral = jnp.transpose(spectral.reshape(band, lons, lon_dev, channels), (1, 0, 2, 3))
    spectral = lax.all_to_all(
        spectral.reshape(lat_dev, lon_dev, channels), "lon", 0, 0, tiled=True
    )
    direct = jnp.dot(
        field.reshape(-1, channels), skip_weight[0], preferred_element_type=f32
    ).reshape(field.shape)
    direct = lax.optimization_barrier(direct.astype(bf16)).astype(f32)
    pre_act = spectral.astype(f32) + direct
    half = 0.5 * pre_act
    advanced = field.astype(f32) + (half + half * lax.erf(pre_act * math.sqrt(0.5)))
    return (advanced.astype(bf16), mixed.reshape(slots, degrees, 2, channels))


def solution(mesh):
    names = ("member", "latx", "core", "lon")
    sizes = dict(mesh.shape)
    chips = Mesh(
        mesh.devices.reshape(sizes["member"], sizes["lat"] // 2, 2, sizes["lon"]), names
    )
    in_specs = (
        P(("member", "latx", "core"), "lon", None),
        P(),
        P(("latx", "core", "lon"), None, None),
        P(("latx", "core", "lon"), None, None),
        P(),
        P(),
        P(),
    )
    out_specs = (
        P(("member", "latx", "core"), "lon", None),
        P(("member", "latx", "core", "lon"), None, None, None),
    )

    return jax.shard_map(
        per_device, mesh=chips, in_specs=in_specs, out_specs=out_specs, check_vma=False
    )
```
